32 devices in a mesh: seq: 8 (over z, y), tensor: 4 (over x, core).
Axes of the slice: x: 2, y: 2, z: 4, core: 2. Of those that a mesh axis runs over, the one named last changes fastest.
Arguments:
- queries: bfloat16 [2048, 8192], P('seq', 'tensor'), may hold values from -4 to 4, as said below
- keys: bfloat16 [2048, 1024], P('seq', 'tensor'), may hold values from -96 to 96, as said below
- values: bfloat16 [2048, 1024], P('seq', 'tensor'), may hold values from -6 to 6
- block_pos: int32 [16], replicated, may hold values from 0 to 15, each once
Outputs:
- attended: bfloat16 [2048, 8192], P('seq')
The draws below stay inside these ranges and needn't reach their ends.
Inputs may be any that keep to these rules, and one draw needn't show every extreme that they name: block_pos is a permutation of 0 to 15. real-valued queries. real-valued keys.
All inputs are finite; a program needn't handle non-finite values.
Results may differ from the reference program's by a relative error of at most 0.004.
Values may be sent and summed in bfloat16 or wider, within the bound.
A program may use at most 64 MiB of HBM per device.

```python
import math
import jax
import jax.numpy as jnp
from jax import lax

QUERY_HEADS = 64
KEY_VALUE_HEADS = 8
HEAD_WIDTH = 128
VISIBLE_SHARDS = 4
SHARD_TOKENS = 256
BLK = 128
NB = 16
SEQUENCE_TOKENS = 2048
N_SEQ = 8


def shared_fields(key):
    base = jax.random.fold_in(key, 7)
    key_q, key_sample = jax.random.split(base, 2)
    query_field = jnp.clip(jax.random.normal(key_q, (SEQUENCE_TOKENS, QUERY_HEADS * HEAD_WIDTH), jnp.float32), -4.0, 4.0)
    key_tensor = jnp.clip(jax.random.normal(key_sample, (SEQUENCE_TOKENS, KEY_VALUE_HEADS * HEAD_WIDTH), jnp.float32), -4.0, 4.0)
    return (query_field, key_tensor)


def draw_queries(key, part):
    return shared_fields(key)[0].astype(jnp.bfloat16)


def draw_keys(key, part):
    return shared_fields(key)[1].astype(jnp.bfloat16)


def block_scale(stream_key, extent, pieces, smallest, top_value):
    loudness, own = 1.0, jax.random.fold_in(stream_key, 6)
    for dim, parts in pieces:
        steps = jnp.exp(jax.random.uniform(jax.random.fold_in(own, dim), (parts,), jnp.float32, smallest / len(pieces), top_value / len(pieces)))
        loudness = loudness * jnp.repeat(steps, extent[dim] // parts).reshape([-1 if axis == dim else 1 for axis in range(len(extent))])
    return loudness


def scatter_about(own_key, extent, width, bound, cuts=(), kind=jnp.bfloat16):
    array = jax.random.normal(own_key, extent, jnp.float32) * width
    if len(cuts) > 0:
        array = block_scale(own_key, extent, cuts, -0.22, 0.18) * array
    return jnp.clip(array, min=-bound, max=bound).astype(kind)


def setup_inputs(seed: int = 0) -> dict:
    seeds = jax.random.split(jax.random.key(seed), 5)
    queries = draw_queries(jax.random.fold_in(seeds[4], 71), 0)
    keys = draw_keys(jax.random.fold_in(seeds[4], 71), 0)
    values = scatter_about(seeds[2], (SEQUENCE_TOKENS, KEY_VALUE_HEADS * HEAD_WIDTH), 1.0, 6.0, ((0, 8), (1, 4)))
    block_pos = jax.random.permutation(seeds[3], NB).astype(jnp.int32)
    return dict(queries=queries, keys=keys, values=values, block_pos=block_pos)


def reference(queries, keys, values, block_pos):
    group_factor = QUERY_HEADS // KEY_VALUE_HEADS
    scale = 1.0 / math.sqrt(HEAD_WIDTH)
    offsets = jnp.arange(BLK, dtype=jnp.int32)
    positions = (block_pos[:, None].astype(jnp.int32) * BLK + offsets[None, :]).reshape(-1)

    def one_shard(shard):
        start = (shard * SHARD_TOKENS).astype(jnp.int32)
        query_rows = lax.dynamic_slice_in_dim(queries, start, SHARD_TOKENS, 0).astype(jnp.float32)
        query_rows = query_rows.reshape(SHARD_TOKENS, KEY_VALUE_HEADS, group_factor, HEAD_WIDTH)
        q_pos = lax.dynamic_slice_in_dim(positions, start, SHARD_TOKENS, 0)
        key_collection = []
        value_collection = []
        pos_list = []
        for back in range(VISIBLE_SHARDS):
            source = ((shard - back) % N_SEQ * SHARD_TOKENS).astype(jnp.int32)
            key_collection.append(lax.dynamic_slice_in_dim(keys, source, SHARD_TOKENS, 0))
            value_collection.append(lax.dynamic_slice_in_dim(values, source, SHARD_TOKENS, 0))
            pos_list.append(lax.dynamic_slice_in_dim(positions, source, SHARD_TOKENS, 0))
        key_gathered = jnp.concatenate(key_collection, 0).astype(jnp.float32).reshape(VISIBLE_SHARDS * SHARD_TOKENS, KEY_VALUE_HEADS, HEAD_WIDTH)
        value_gathered = jnp.concatenate(value_collection, 0).astype(jnp.float32).reshape(VISIBLE_SHARDS * SHARD_TOKENS, KEY_VALUE_HEADS, HEAD_WIDTH)
        key_pos = jnp.concatenate(pos_list, 0)
        scores = jnp.einsum('qgrd,kgd->grqk', query_rows, key_gathered) * scale
        allowed = key_pos[None, :] <= q_pos[:, None]
        scores = jnp.where(allowed[None, None], scores, -1e+30)
        top = lax.optimization_barrier(jnp.max(scores, axis=-1, keepdims=True))
        weights = jnp.exp(scores - top)
        total = lax.optimization_barrier(jnp.sum(weights, axis=-1))
        rounded = lax.optimization_barrier(weights.astype(jnp.bfloat16)).astype(jnp.float32)
        mixed = jnp.einsum('grqk,kgd->qgrd', rounded, value_gathered)
        mixed = mixed / jnp.transpose(total, (2, 0, 1))[..., None]
        return mixed.reshape(SHARD_TOKENS, QUERY_HEADS * HEAD_WIDTH).astype(jnp.bfloat16)
    shards = lax.map(one_shard, jnp.arange(N_SEQ, dtype=jnp.int32))
    return shards.reshape(SEQUENCE_TOKENS, QUERY_HEADS * HEAD_WIDTH)
```

```python
import functools
import math

import jax
import jax.numpy as jnp
from jax import lax
from jax.experimental import pallas as pl
from jax.experimental.pallas import tpu as pltpu
from jax.sharding import PartitionSpec as P

HEAD = 128
GROUP = 8
WINDOW = 4
MESH = pl.DeviceIdType.MESH


def kernel(n, T, rows, groups, q_hbm, k_hbm, v_hbm, bp, out, qv, kv, bias,
           ld_sem, kv_send, kv_recv, x_send, x_recv, c_send, c_recv):
    s = lax.axis_index("seq")
    t = lax.axis_index("tensor")
    heads = groups * GROUP
    hops = T // 2 - 1
    half = rows // 2

    def seq_dev(d):
        return (lax.rem(s + d + n, n), t)

    def x_dev(k):
        return (s, lax.rem(t + 2 * k + T, T))

    sibling = (s, t + 1 - 2 * lax.rem(t, 2))

    loads = []
    for g in range(groups):
        cols = pl.ds(g * HEAD, HEAD)
        pair = []
        for i, src in enumerate((k_hbm, v_hbm)):
            c = pltpu.make_async_copy(src.at[:, cols], kv.at[g, 0, i], ld_sem.at[g, i])
            c.start()
            pair.append(c)
        loads.append(pair)
    q_load = pltpu.make_async_copy(q_hbm, qv, ld_sem.at[groups, 0])
    q_load.start()

    barrier = pltpu.get_barrier_semaphore()
    peers = [seq_dev(d) for d in (1, 2, 3, -1, -2, -3)] + [sibling]
    peers += [x_dev(k) for k in range(1, hops + 1)]
    for p in peers:
        pl.semaphore_signal(barrier, inc=1, device_id=p, device_id_type=MESH)
    pl.semaphore_wait(barrier, len(peers))

    def kv_copy(g, b):
        return pltpu.make_async_remote_copy(
            src_ref=kv.at[g, 0], dst_ref=kv.at[g, b],
            send_sem=kv_send.at[g, b - 1], recv_sem=kv_recv.at[g, b - 1],
            device_id=seq_dev(b), device_id_type=MESH)

    for g in range(groups):
        for c in loads[g]:
            c.wait()
        for b in (3, 2, 1):
            kv_copy(g, b).start()

    blk = half
    lane = lax.broadcasted_iota(jnp.int32, (blk, blk), 1)
    sub = lax.broadcasted_iota(jnp.int32, (blk, blk), 0)
    for i in range(2):
        qpos = bp[2 * s + i] * blk + sub
        for b in range(WINDOW):
            owner = lax.rem(s - b + n, n)
            for j in range(2):
                kpos = bp[2 * owner + j] * blk + lane
                bias[i * blk:(i + 1) * blk, (2 * b + j) * blk:(2 * b + j + 1) * blk] = (
                    jnp.where(kpos <= qpos, 0.0, -1e30).astype(jnp.float32))
    q_load.wait()

    def piece(owner, h):
        col = pl.multiple_of((owner * heads + h) * HEAD, HEAD)
        return out.at[:, pl.ds(col, HEAD)]

    def x_copy(k, h, owner):
        return pltpu.make_async_remote_copy(
            src_ref=piece(owner, h), dst_ref=piece(owner, h),
            send_sem=x_send.at[k - 1, h], recv_sem=x_recv.at[k - 1, h],
            device_id=x_dev(k), device_id_type=MESH)

    def c_copy(k, h, owner):
        return pltpu.make_async_remote_copy(
            src_ref=piece(owner, h), dst_ref=piece(owner, h),
            send_sem=c_send.at[k, h], recv_sem=c_recv.at[k, h],
            device_id=sibling, device_id_type=MESH)

    factor = math.log2(math.e) / math.sqrt(HEAD)
    window = WINDOW * rows

    for g in range(groups):
        for b in (1, 2, 3):
            kv_copy(g, b).wait_recv()

        def one_head(r, _, g=g):
            h = g * GROUP + r
            qcol = pl.multiple_of(h * HEAD, HEAD)
            ocol = pl.multiple_of((t * heads + h) * HEAD, HEAD)
            keys = kv[g, :, 0].reshape(window, HEAD)
            vals = kv[g, :, 1].reshape(window, HEAD)
            for i in range(2):
                part = slice(i * half, (i + 1) * half)
                q = qv[part, pl.ds(qcol, HEAD)]
                sc = lax.dot_general(q, keys, (((1,), (1,)), ((), ())),
                                     preferred_element_type=jnp.float32)
                sc = sc + bias[part, :]
                top = jnp.max(sc, axis=1, keepdims=True)
                w = jnp.exp2((sc - top) * factor)
                total = jnp.sum(w, axis=1, keepdims=True)
                mixed = jnp.dot(w.astype(jnp.bfloat16), vals,
                                preferred_element_type=jnp.float32)
                out[part, pl.ds(ocol, HEAD)] = (mixed / total).astype(out.dtype)
            for k in range(1, hops + 1):
                x_copy(k, h, t).start()
            c_copy(0, h, t).start()
            return 0

        lax.fori_loop(0, GROUP, one_head, 0)

    def forward(h, _):
        for k in range(1, hops + 1):
            owner = lax.rem(t - 2 * k + T, T)
            x_copy(k, h, owner).wait_recv()
            c_copy(k, h, owner).start()
        return 0

    lax.fori_loop(0, heads, forward, 0)

    def finish(h, _):
        for k in range(hops + 1):
            c_copy(k, h, t).wait()
            if k > 0:
                x_copy(k, h, t).wait_send()
        return 0

    lax.fori_loop(0, heads, finish, 0)
    for g in range(groups):
        for b in (1, 2, 3):
            kv_copy(g, b).wait_send()


def body(n, T, queries, keys, values, block_pos):
    rows = queries.shape[0]
    groups = keys.shape[1] // HEAD
    heads = groups * GROUP
    hops = T // 2 - 1
    dma = pltpu.SemaphoreType.DMA
    return pl.pallas_call(
        functools.partial(kernel, n, T, rows, groups),
        out_shape=jax.ShapeDtypeStruct((rows, queries.shape[1] * T), jnp.bfloat16),
        in_specs=[pl.BlockSpec(memory_space=pltpu.HBM)] * 3
        + [pl.BlockSpec(memory_space=pltpu.SMEM)],
        out_specs=pl.BlockSpec(memory_space=pltpu.VMEM),
        scratch_shapes=[
            pltpu.VMEM((rows, heads * HEAD), jnp.bfloat16),
            pltpu.VMEM((groups, WINDOW, 2, rows, HEAD), jnp.bfloat16),
            pltpu.VMEM((rows, WINDOW * rows), jnp.float32),
            dma((groups + 1, 2)),
            dma((groups, 3)),
            dma((groups, 3)),
            dma((hops, heads)),
            dma((hops, heads)),
            dma((hops + 1, heads)),
            dma((hops + 1, heads)),
        ],
        compiler_params=pltpu.CompilerParams(
            collective_id=0, has_side_effects=True, vmem_limit_bytes=32 * 1024 * 1024),
    )(queries, keys, values, block_pos)


def solution(mesh):
    n, T = mesh.shape["seq"], mesh.shape["tensor"]
    placed = (P("seq", "tensor"), P("seq", "tensor"), P("seq", "tensor"), P())
    return jax.shard_map(functools.partial(body, n, T), mesh=mesh, in_specs=placed,
                         out_specs=P("seq", None), check_vma=False)
```

```python
import functools
import math

import jax
import jax.numpy as jnp
from jax import lax
from jax.experimental import pallas as pl
from jax.experimental.pallas import tpu as pltpu
from jax.sharding import PartitionSpec as P

HEAD = 128
GROUP = 8
WINDOW = 4
MESH = pl.DeviceIdType.MESH


def kernel(n, T, rows, groups, q_hbm, k_hbm, v_hbm, bp_hbm, out, bp, qv, kv, bias,
           ld_sem, kv_send, kv_recv, x_send, x_recv, c_send, c_recv):
    s = lax.axis_index("seq")
    t = lax.axis_index("tensor")
    heads = groups * GROUP
    hops = T // 2 - 1
    half = rows // 2

    def seq_dev(d):
        return (lax.rem(s + d + n, n), t)

    def x_dev(k):
        return (s, lax.rem(t + 2 * k + T, T))

    sibling = (s, t + 1 - 2 * lax.rem(t, 2))

    loads = []
    for g in range(groups):
        cols = pl.ds(g * HEAD, HEAD)
        pair = []
        for i, src in enumerate((k_hbm, v_hbm)):
            c = pltpu.make_async_copy(src.at[:, cols], kv.at[g, 0, i], ld_sem.at[g, i])
            c.start()
            pair.append(c)
        loads.append(pair)
    q_load = pltpu.make_async_copy(q_hbm, qv, ld_sem.at[groups, 0])
    q_load.start()
    bp_load = pltpu.make_async_copy(bp_hbm, bp, ld_sem.at[groups, 1])
    bp_load.start()

    barrier = pltpu.get_barrier_semaphore()
    peers = [seq_dev(d) for d in (1, 2, -1, -2)] + [sibling]
    peers += [x_dev(k) for k in range(1, hops + 1)]
    for p in peers:
        pl.semaphore_signal(barrier, inc=1, device_id=p, device_id_type=MESH)
    pl.semaphore_wait(barrier, len(peers))

    odd = lax.rem(s, 2)

    def kv_copy(g, i, b, src, d):
        return pltpu.make_async_remote_copy(
            src_ref=kv.at[g, src, i], dst_ref=kv.at[g, b, i],
            send_sem=kv_send.at[g, i, b - 1], recv_sem=kv_recv.at[g, i, b - 1],
            device_id=seq_dev(d), device_id_type=MESH)

    def two(g, i):
        return kv_copy(g, i, 2, 0, 2)

    def three(g, i):
        return kv_copy(g, i, 3, 2, 1)

    def send_own(g):
        for i in range(2):
            loads[g][i].wait()
            two(g, i).start()

            @pl.when(odd == 0)
            def _():
                kv_copy(g, i, 1, 0, 1).start()

    def send_on(g):
        for i in range(2):
            two(g, i).wait_recv()

            @pl.when(odd == 1)
            def _():
                kv_copy(g, i, 1, 2, -1).start()

            three(g, i).start()

    send_own(0)
    bp_load.wait()
    blk = half
    lane = lax.broadcasted_iota(jnp.int32, (blk, blk), 1)
    sub = lax.broadcasted_iota(jnp.int32, (blk, blk), 0)
    for i in range(2):
        qpos = bp[2 * s + i] * blk + sub
        for b in range(WINDOW):
            owner = lax.rem(s - b + n, n)
            for j in range(2):
                kpos = bp[2 * owner + j] * blk + lane
                bias[i * blk:(i + 1) * blk, (2 * b + j) * blk:(2 * b + j + 1) * blk] = (
                    jnp.where(kpos <= qpos, 0.0, -1e30).astype(jnp.float32))
    q_load.wait()
    send_on(0)
    for g in range(1, groups):
        send_own(g)

    def piece(owner, h):
        col = pl.multiple_of((owner * heads + h) * HEAD, HEAD)
        return out.at[:, pl.ds(col, HEAD)]

    def x_copy(k, h, owner):
        return pltpu.make_async_remote_copy(
            src_ref=piece(owner, h), dst_ref=piece(owner, h),
            send_sem=x_send.at[k - 1, h], recv_sem=x_recv.at[k - 1, h],
            device_id=x_dev(k), device_id_type=MESH)

    def c_copy(k, h, owner):
        return pltpu.make_async_remote_copy(
            src_ref=piece(owner, h), dst_ref=piece(owner, h),
            send_sem=c_send.at[k, h], recv_sem=c_recv.at[k, h],
            device_id=sibling, device_id_type=MESH)

    factor = math.log2(math.e) / math.sqrt(HEAD)
    window = WINDOW * rows

    for g in range(groups):
        for i in range(2):
            kv_copy(g, i, 1, 0, 1).wait_recv()
            three(g, i).wait_recv()

        def one_head(r, _, g=g):
            h = g * GROUP + r
            qcol = pl.multiple_of(h * HEAD, HEAD)
            ocol = pl.multiple_of((t * heads + h) * HEAD, HEAD)
            keys = kv[g, :, 0].reshape(window, HEAD)
            vals = kv[g, :, 1].reshape(window, HEAD)
            for i in range(2):
                part = slice(i * half, (i + 1) * half)
                q = qv[part, pl.ds(qcol, HEAD)]
                sc = lax.dot_general(q, keys, (((1,), (1,)), ((), ())),
                                     preferred_element_type=jnp.float32)
                sc = sc + bias[part, :]
                top = jnp.max(sc, axis=1, keepdims=True)
                w = jnp.exp2((sc - top) * factor)
                total = jnp.sum(w, axis=1, keepdims=True)
                mixed = jnp.dot(w.astype(jnp.bfloat16), vals,
                                preferred_element_type=jnp.float32)
                out[part, pl.ds(ocol, HEAD)] = (mixed / total).astype(out.dtype)
            for k in range(1, hops + 1):
                x_copy(k, h, t).start()
            c_copy(0, h, t).start()
            return 0

        lax.fori_loop(0, GROUP // 2, one_head, 0)
        if g + 1 < groups:
            send_on(g + 1)
        lax.fori_loop(GROUP // 2, GROUP, one_head, 0)

    def forward(h, _):
        for k in range(1, hops + 1):
            owner = lax.rem(t - 2 * k + T, T)
            x_copy(k, h, owner).wait_recv()
            c_copy(k, h, owner).start()
        return 0

    lax.fori_loop(0, heads, forward, 0)

    def finish(h, _):
        for k in range(hops + 1):
            c_copy(k, h, t).wait()
            if k > 0:
                x_copy(k, h, t).wait_send()
        return 0

    lax.fori_loop(0, heads, finish, 0)
    for g in range(groups):
        for i in range(2):
            kv_copy(g, i, 1, 0, 1).wait_send()
            two(g, i).wait_send()
            three(g, i).wait_send()


def body(n, T, queries, keys, values, block_pos):
    rows = queries.shape[0]
    groups = keys.shape[1] // HEAD
    heads = groups * GROUP
    hops = T // 2 - 1
    dma = pltpu.SemaphoreType.DMA
    return pl.pallas_call(
        functools.partial(kernel, n, T, rows, groups),
        out_shape=jax.ShapeDtypeStruct((rows, queries.shape[1] * T), jnp.bfloat16),
        in_specs=[pl.BlockSpec(memory_space=pltpu.HBM)] * 4,
        out_specs=pl.BlockSpec(memory_space=pltpu.VMEM),
        scratch_shapes=[
            pltpu.SMEM(block_pos.shape, jnp.int32),
            pltpu.VMEM((rows, heads * HEAD), jnp.bfloat16),
            pltpu.VMEM((groups, WINDOW, 2, rows, HEAD), jnp.bfloat16),
            pltpu.VMEM((rows, WINDOW * rows), jnp.float32),
            dma((groups + 1, 2)),
            dma((groups, 2, 3)),
            dma((groups, 2, 3)),
            dma((hops, heads)),
            dma((hops, heads)),
            dma((hops + 1, heads)),
            dma((hops + 1, heads)),
        ],
        compiler_params=pltpu.CompilerParams(
            collective_id=0, has_side_effects=True, vmem_limit_bytes=32 * 1024 * 1024),
    )(*(pltpu.with_memory_space_constraint(z, pltpu.HBM)
        for z in (queries, keys, values, block_pos)))


def solution(mesh):
    n, T = mesh.shape["seq"], mesh.shape["tensor"]
    placed = (P("seq", "tensor"), P("seq", "tensor"), P("seq", "tensor"), P())
    return jax.shard_map(functools.partial(body, n, T), mesh=mesh, in_specs=placed,
                         out_specs=P("seq", None), check_vma=False)
```

```python
import functools
import math

import jax
import jax.numpy as jnp
from jax import lax
from jax.experimental import pallas as pl
from jax.experimental.pallas import tpu as pltpu
from jax.sharding import PartitionSpec as P

HEAD = 128
GROUP = 8
CUTS = 2
WINDOW = 4
MESH = pl.DeviceIdType.MESH


def kernel(n, T, rows, groups, q_hbm, k_hbm, v_hbm, bp_hbm, out, bp, qv, kv, bias,
           ld_sem, kv_send, kv_recv, x_send, x_recv, c_send, c_recv):
    s = lax.axis_index("seq")
    t = lax.axis_index("tensor")
    heads = groups * GROUP
    hops = T // 2 - 1
    half = rows // 2

    def seq_dev(d):
        return (lax.rem(s + d + n, n), t)

    def x_dev(k):
        return (s, lax.rem(t + 2 * k + T, T))

    sibling = (s, t + 1 - 2 * lax.rem(t, 2))

    loads = []
    for g in range(groups):
        cols = pl.ds(g * HEAD, HEAD)
        pair = []
        for i, src in enumerate((k_hbm, v_hbm)):
            c = pltpu.make_async_copy(src.at[:, cols], kv.at[g, 0, i], ld_sem.at[g, i])
            c.start()
            pair.append(c)
        loads.append(pair)
    q_load = pltpu.make_async_copy(q_hbm, qv, ld_sem.at[groups, 0])
    q_load.start()
    bp_load = pltpu.make_async_copy(bp_hbm, bp, ld_sem.at[groups, 1])
    bp_load.start()

    barrier = pltpu.get_barrier_semaphore()
    peers = [seq_dev(d) for d in (1, 2, -1, -2)] + [sibling]
    peers += [x_dev(k) for k in range(1, hops + 1)]
    for p in peers:
        pl.semaphore_signal(barrier, inc=1, device_id=p, device_id_type=MESH)
    pl.semaphore_wait(barrier, len(peers))

    odd = lax.rem(s, 2)

    cut = rows // CUTS

    def kv_copy(g, i, b, src, d):
        part = pl.ds(i % CUTS * cut, cut)
        return pltpu.make_async_remote_copy(
            src_ref=kv.at[g, src, i // CUTS, part], dst_ref=kv.at[g, b, i // CUTS, part],
            send_sem=kv_send.at[g, i, b - 1], recv_sem=kv_recv.at[g, i, b - 1],
            device_id=seq_dev(d), device_id_type=MESH)

    def two(g, i):
        return kv_copy(g, i, 2, 0, 2)

    def three(g, i):
        return kv_copy(g, i, 3, 2, 1)

    def send_own(g):
        for i in range(2 * CUTS):
            if i % CUTS == 0:
                loads[g][i // CUTS].wait()
            two(g, i).start()

            @pl.when(odd == 0)
            def _():
                kv_copy(g, i, 1, 0, 1).start()

    def send_on(g):
        for i in range(2 * CUTS):
            two(g, i).wait_recv()

            @pl.when(odd == 1)
            def _():
                kv_copy(g, i, 1, 2, -1).start()

            three(g, i).start()

    send_own(0)
    bp_load.wait()
    blk = half
    lane = lax.broadcasted_iota(jnp.int32, (blk, blk), 1)
    sub = lax.broadcasted_iota(jnp.int32, (blk, blk), 0)
    for i in range(2):
        qpos = bp[2 * s + i] * blk + sub
        for b in range(WINDOW):
            owner = lax.rem(s - b + n, n)
            for j in range(2):
                kpos = bp[2 * owner + j] * blk + lane
                bias[i * blk:(i + 1) * blk, (2 * b + j) * blk:(2 * b + j + 1) * blk] = (
                    jnp.where(kpos <= qpos, 0.0, -1e30).astype(jnp.float32))
    q_load.wait()
    send_on(0)
    for g in range(1, groups):
        send_own(g)

    def piece(owner, h):
        col = pl.multiple_of((owner * heads + h) * HEAD, HEAD)
        return out.at[:, pl.ds(col, HEAD)]

    def x_copy(k, h, owner):
        return pltpu.make_async_remote_copy(
            src_ref=piece(owner, h), dst_ref=piece(owner, h),
            send_sem=x_send.at[k - 1, h], recv_sem=x_recv.at[k - 1, h],
            device_id=x_dev(k), device_id_type=MESH)

    def c_copy(k, h, owner):
        return pltpu.make_async_remote_copy(
            src_ref=piece(owner, h), dst_ref=piece(owner, h),
            send_sem=c_send.at[k, h], recv_sem=c_recv.at[k, h],
            device_id=sibling, device_id_type=MESH)

    factor = math.log2(math.e) / math.sqrt(HEAD)
    window = WINDOW * rows

    for g in range(groups):
        for i in range(2 * CUTS):
            kv_copy(g, i, 1, 0, 1).wait_recv()
            three(g, i).wait_recv()

        def one_head(r, _, g=g):
            h = g * GROUP + r
            qcol = pl.multiple_of(h * HEAD, HEAD)
            ocol = pl.multiple_of((t * heads + h) * HEAD, HEAD)
            keys = kv[g, :, 0].reshape(window, HEAD)
            vals = kv[g, :, 1].reshape(window, HEAD)
            for i in range(2):
                part = slice(i * half, (i + 1) * half)
                q = qv[part, pl.ds(qcol, HEAD)]
                sc = lax.dot_general(q, keys, (((1,), (1,)), ((), ())),
                                     preferred_element_type=jnp.float32)
                sc = sc + bias[part, :]
                top = jnp.max(sc, axis=1, keepdims=True)
                w = jnp.exp2((sc - top) * factor)
                total = jnp.sum(w, axis=1, keepdims=True)
                mixed = jnp.dot(w.astype(jnp.bfloat16), vals,
                                preferred_element_type=jnp.float32)
                out[part, pl.ds(ocol, HEAD)] = (mixed / total).astype(out.dtype)
            for k in range(1, hops + 1):
                x_copy(k, h, t).start()
            c_copy(0, h, t).start()
            return 0

        lax.fori_loop(0, GROUP // 2, one_head, 0)
        if g + 1 < groups:
            send_on(g + 1)
        lax.fori_loop(GROUP // 2, GROUP, one_head, 0)

    def forward(h, _):
        for k in range(1, hops + 1):
            owner = lax.rem(t - 2 * k + T, T)
            x_copy(k, h, owner).wait_recv()
            c_copy(k, h, owner).start()
        return 0

    lax.fori_loop(0, heads, forward, 0)

    def finish(h, _):
        for k in range(hops + 1):
            c_copy(k, h, t).wait()
            if k > 0:
                x_copy(k, h, t).wait_send()
        return 0

    lax.fori_loop(0, heads, finish, 0)
    for g in range(groups):
        for i in range(2 * CUTS):
            kv_copy(g, i, 1, 0, 1).wait_send()
            two(g, i).wait_send()
            three(g, i).wait_send()


def body(n, T, queries, keys, values, block_pos):
    rows = queries.shape[0]
    groups = keys.shape[1] // HEAD
    heads = groups * GROUP
    hops = T // 2 - 1
    dma = pltpu.SemaphoreType.DMA
    return pl.pallas_call(
        functools.partial(kernel, n, T, rows, groups),
        out_shape=jax.ShapeDtypeStruct((rows, queries.shape[1] * T), jnp.bfloat16),
        in_specs=[pl.BlockSpec(memory_space=pltpu.HBM)] * 4,
        out_specs=pl.BlockSpec(memory_space=pltpu.VMEM),
        scratch_shapes=[
            pltpu.SMEM(block_pos.shape, jnp.int32),
            pltpu.VMEM((rows, heads * HEAD), jnp.bfloat16),
            pltpu.VMEM((groups, WINDOW, 2, rows, HEAD), jnp.bfloat16),
            pltpu.VMEM((rows, WINDOW * rows), jnp.float32),
            dma((groups + 1, 2)),
            dma((groups, 2 * CUTS, 3)),
            dma((groups, 2 * CUTS, 3)),
            dma((hops, heads)),
            dma((hops, heads)),
            dma((hops + 1, heads)),
            dma((hops + 1, heads)),
        ],
        compiler_params=pltpu.CompilerParams(
            collective_id=0, has_side_effects=True, vmem_limit_bytes=32 * 1024 * 1024),
    )(*(pltpu.with_memory_space_constraint(z, pltpu.HBM)
        for z in (queries, keys, values, block_pos)))


def solution(mesh):
    n, T = mesh.shape["seq"], mesh.shape["tensor"]
    placed = (P("seq", "tensor"), P("seq", "tensor"), P("seq", "tensor"), P())
    return jax.shard_map(functools.partial(body, n, T), mesh=mesh, in_specs=placed,
                         out_specs=P("seq", None), check_vma=False)
```

```python
import functools
import math

import jax
import jax.numpy as jnp
from jax import lax
from jax.experimental import pallas as pl
from jax.experimental.pallas import tpu as pltpu
from jax.sharding import PartitionSpec as P

HEAD = 128
GROUP = 8
CUTS = 2
WINDOW = 4
MESH = pl.DeviceIdType.MESH


def kernel(n, T, rows, groups, q_hbm, k_hbm, v_hbm, bp_hbm, out, bp, qv, kv, bias,
           ld_sem, kv_send, kv_recv, x_send, x_recv, c_send, c_recv):
    s = lax.axis_index("seq")
    t = lax.axis_index("tensor")
    heads = groups * GROUP
    hops = T // 2 - 1
    half = rows // 2

    def seq_dev(d):
        return (lax.rem(s + d + n, n), t)

    def x_dev(k):
        return (s, lax.rem(t + 2 * k + T, T))

    sibling = (s, t + 1 - 2 * lax.rem(t, 2))

    loads = []
    for g in range(groups):
        cols = pl.ds(g * HEAD, HEAD)
        pair = []
        for i, src in enumerate((k_hbm, v_hbm)):
            c = pltpu.make_async_copy(src.at[:, cols], kv.at[g, 0, i], ld_sem.at[g, i])
            c.start()
            pair.append(c)
        loads.append(pair)
    q_load = pltpu.make_async_copy(q_hbm, qv, ld_sem.at[groups, 0])
    q_load.start()
    bp_load = pltpu.make_async_copy(bp_hbm, bp, ld_sem.at[groups, 1])
    bp_load.start()

    barrier = pltpu.get_barrier_semaphore()
    peers = [seq_dev(d) for d in (1, 2, -1, -2)] + [sibling]
    peers += [x_dev(k) for k in range(1, hops + 1)]
    for p in peers:
        pl.semaphore_signal(barrier, inc=1, device_id=p, device_id_type=MESH)
    pl.semaphore_wait(barrier, len(peers))

    odd = lax.rem(s, 2)

    cut = rows // CUTS

    def kv_copy(g, i, b, src, d):
        part = pl.ds(i % CUTS * cut, cut)
        return pltpu.make_async_remote_copy(
            src_ref=kv.at[g, src, i // CUTS, part], dst_ref=kv.at[g, b, i // CUTS, part],
            send_sem=kv_send.at[g, i, b - 1], recv_sem=kv_recv.at[g, i, b - 1],
            device_id=seq_dev(d), device_id_type=MESH)

    def two(g, i):
        return kv_copy(g, i, 2, 0, 2)

    def three(g, i):
        return kv_copy(g, i, 3, 2, 1)

    def send_own(g):
        for i in range(2 * CUTS):
            if i % CUTS == 0:
                loads[g][i // CUTS].wait()
            two(g, i).start()

            @pl.when(odd == 0)
            def _():
                kv_copy(g, i, 1, 0, 1).start()

    def send_on(g):
        for i in range(2 * CUTS):
            two(g, i).wait_recv()

            @pl.when(odd == 1)
            def _():
                kv_copy(g, i, 1, 2, -1).start()

            three(g, i).start()

    send_own(0)
    bp_load.wait()
    blk = half
    lane = lax.broadcasted_iota(jnp.int32, (blk, blk), 1)
    sub = lax.broadcasted_iota(jnp.int32, (blk, blk), 0)
    for i in range(2):
        qpos = bp[2 * s + i] * blk + sub
        for b in range(WINDOW):
            owner = lax.rem(s - b + n, n)
            for j in range(2):
                kpos = bp[2 * owner + j] * blk + lane
                bias[i * blk:(i + 1) * blk, (2 * b + j) * blk:(2 * b + j + 1) * blk] = (
                    jnp.where(kpos <= qpos, 0.0, -1e30).astype(jnp.float32))
    q_load.wait()
    send_on(0)
    for g in range(1, groups):
        send_own(g)

    def piece(owner, h):
        col = pl.multiple_of((owner * heads + h) * HEAD, HEAD)
        return out.at[:, pl.ds(col, HEAD)]

    def x_copy(k, h, owner):
        return pltpu.make_async_remote_copy(
            src_ref=piece(owner, h), dst_ref=piece(owner, h),
            send_sem=x_send.at[k - 1, h], recv_sem=x_recv.at[k - 1, h],
            device_id=x_dev(k), device_id_type=MESH)

    def c_copy(k, h, owner):
        return pltpu.make_async_remote_copy(
            src_ref=piece(owner, h), dst_ref=piece(owner, h),
            send_sem=c_send.at[k, h], recv_sem=c_recv.at[k, h],
            device_id=sibling, device_id_type=MESH)

    factor = math.log2(math.e) / math.sqrt(HEAD)
    window = WINDOW * rows

    for g in range(groups):
        def arrive(which, g=g):
            for i in range(which * CUTS, (which + 1) * CUTS):
                kv_copy(g, i, 1, 0, 1).wait_recv()
                three(g, i).wait_recv()

        arrive(0)

        def one_head(r, _, g=g, late=None):
            h = g * GROUP + r
            qcol = pl.multiple_of(h * HEAD, HEAD)
            ocol = pl.multiple_of((t * heads + h) * HEAD, HEAD)
            keys = kv[g, :, 0].reshape(window, HEAD)
            made = []
            for i in range(2):
                part = slice(i * half, (i + 1) * half)
                q = qv[part, pl.ds(qcol, HEAD)]
                sc = lax.dot_general(q, keys, (((1,), (1,)), ((), ())),
                                     preferred_element_type=jnp.float32)
                sc = sc + bias[part, :]
                top = jnp.max(sc, axis=1, keepdims=True)
                w = jnp.exp2((sc - top) * factor)
                total = jnp.sum(w, axis=1, keepdims=True)
                made.append((part, w.astype(jnp.bfloat16), total))
            if late is not None:
                late(1)
            vals = kv[g, :, 1].reshape(window, HEAD)
            for part, w, total in made:
                mixed = jnp.dot(w, vals, preferred_element_type=jnp.float32)
                out[part, pl.ds(ocol, HEAD)] = (mixed / total).astype(out.dtype)
            for k in range(1, hops + 1):
                x_copy(k, h, t).start()
            c_copy(0, h, t).start()
            return 0

        one_head(0, 0, late=arrive)
        lax.fori_loop(1, GROUP // 2, one_head, 0)
        if g + 1 < groups:
            send_on(g + 1)
        lax.fori_loop(GROUP // 2, GROUP, one_head, 0)

    def forward(h, _):
        for k in range(1, hops + 1):
            owner = lax.rem(t - 2 * k + T, T)
            x_copy(k, h, owner).wait_recv()
            c_copy(k, h, owner).start()
        return 0

    lax.fori_loop(0, heads, forward, 0)

    def finish(h, _):
        for k in range(hops + 1):
            c_copy(k, h, t).wait()
            if k > 0:
                x_copy(k, h, t).wait_send()
        return 0

    lax.fori_loop(0, heads, finish, 0)
    for g in range(groups):
        for i in range(2 * CUTS):
            kv_copy(g, i, 1, 0, 1).wait_send()
            two(g, i).wait_send()
            three(g, i).wait_send()


def body(n, T, queries, keys, values, block_pos):
    rows = queries.shape[0]
    groups = keys.shape[1] // HEAD
    heads = groups * GROUP
    hops = T // 2 - 1
    dma = pltpu.SemaphoreType.DMA
    return pl.pallas_call(
        functools.partial(kernel, n, T, rows, groups),
        out_shape=jax.ShapeDtypeStruct((rows, queries.shape[1] * T), jnp.bfloat16),
        in_specs=[pl.BlockSpec(memory_space=pltpu.HBM)] * 4,
        out_specs=pl.BlockSpec(memory_space=pltpu.VMEM),
        scratch_shapes=[
            pltpu.SMEM(block_pos.shape, jnp.int32),
            pltpu.VMEM((rows, heads * HEAD), jnp.bfloat16),
            pltpu.VMEM((groups, WINDOW, 2, rows, HEAD), jnp.bfloat16),
            pltpu.VMEM((rows, WINDOW * rows), jnp.float32),
            dma((groups + 1, 2)),
            dma((groups, 2 * CUTS, 3)),
            dma((groups, 2 * CUTS, 3)),
            dma((hops, heads)),
            dma((hops, heads)),
            dma((hops + 1, heads)),
            dma((hops + 1, heads)),
        ],
        compiler_params=pltpu.CompilerParams(
            collective_id=0, has_side_effects=True, vmem_limit_bytes=32 * 1024 * 1024),
    )(*(pltpu.with_memory_space_constraint(z, pltpu.HBM)
        for z in (queries, keys, values, block_pos)))


def solution(mesh):
    n, T = mesh.shape["seq"], mesh.shape["tensor"]
    placed = (P("seq", "tensor"), P("seq", "tensor"), P("seq", "tensor"), P())
    return jax.shard_map(functools.partial(body, n, T), mesh=mesh, in_specs=placed,
                         out_specs=P("seq", None), check_vma=False)
```

```python
import functools
import math

import jax
import jax.numpy as jnp
from jax import lax
from jax.experimental import pallas as pl
from jax.experimental.pallas import tpu as pltpu
from jax.sharding import PartitionSpec as P

HEAD = 128
GROUP = 8
CUTS = 2
WINDOW = 4
MESH = pl.DeviceIdType.MESH


def kernel(n, T, rows, groups, q_hbm, k_hbm, v_hbm, bp_hbm, out, bp, qv, kv, bias,
           ld_sem, kv_send, kv_recv, x_send, x_recv, c_send, c_recv):
    s = lax.axis_index("seq")
    t = lax.axis_index("tensor")
    heads = groups * GROUP
    hops = T // 2 - 1
    half = rows // 2

    def seq_dev(d):
        return (lax.rem(s + d + n, n), t)

    def x_dev(k):
        return (s, lax.rem(t + 2 * k + T, T))

    sibling = (s, t + 1 - 2 * lax.rem(t, 2))

    loads = []
    for g in range(groups):
        cols = pl.ds(g * HEAD, HEAD)
        pair = []
        for i, src in enumerate((k_hbm, v_hbm)):
            c = pltpu.make_async_copy(src.at[:, cols], kv.at[g, 0, i], ld_sem.at[g, i])
            c.start()
            pair.append(c)
        loads.append(pair)
    q_load = pltpu.make_async_copy(q_hbm, qv, ld_sem.at[groups, 0])
    q_load.start()
    bp_load = pltpu.make_async_copy(bp_hbm, bp, ld_sem.at[groups, 1])
    bp_load.start()

    barrier = pltpu.get_barrier_semaphore()
    peers = [seq_dev(d) for d in (1, 2, -1, -2)] + [sibling]
    peers += [x_dev(k) for k in range(1, hops + 1)]
    for p in peers:
        pl.semaphore_signal(barrier, inc=1, device_id=p, device_id_type=MESH)
    pl.semaphore_wait(barrier, len(peers))

    odd = lax.rem(s, 2)

    cut = rows // CUTS

    def kv_copy(g, i, b, src, d, sent=None):
        part = pl.ds(i % CUTS * cut, cut)
        return pltpu.make_async_remote_copy(
            src_ref=kv.at[g, src, i // CUTS, part], dst_ref=kv.at[g, b, i // CUTS, part],
            send_sem=kv_send.at[g, i, b - 1 if sent is None else sent], recv_sem=kv_recv.at[g, i, b - 1],
            device_id=seq_dev(d), device_id_type=MESH)

    def two(g, i):
        return kv_copy(g, i, 2, 0, 2)

    def three(g, i):
        return kv_copy(g, i, 3, 2, 1)

    def send_own(g):
        for i in range(2 * CUTS):
            if i % CUTS == 0:
                loads[g][i // CUTS].wait()
            two(g, i).start()

            @pl.when(odd == 0)
            def _():
                kv_copy(g, i, 1, 0, 1).start()

    def send_on(g):
        for i in range(2 * CUTS):
            two(g, i).wait_recv()

            @pl.when(odd == 1)
            def _():
                kv_copy(g, i, 1, 2, -1).start()
                three(g, i).start()
                if i % 2:
                    kv_copy(g, i, 1, 0, 1).wait_recv()
                    kv_copy(g, i, 3, 1, 2, 3).start()

            if i % 2 == 0:
                @pl.when(odd == 0)
                def _():
                    three(g, i).start()

    send_own(0)
    bp_load.wait()
    blk = half
    lane = lax.broadcasted_iota(jnp.int32, (blk, blk), 1)
    sub = lax.broadcasted_iota(jnp.int32, (blk, blk), 0)
    for i in range(2):
        qpos = bp[2 * s + i] * blk + sub
        for b in range(WINDOW):
            owner = lax.rem(s - b + n, n)
            for j in range(2):
                kpos = bp[2 * owner + j] * blk + lane
                bias[i * blk:(i + 1) * blk, (2 * b + j) * blk:(2 * b + j + 1) * blk] = (
                    jnp.where(kpos <= qpos, 0.0, -1e30).astype(jnp.float32))
    q_load.wait()
    send_on(0)
    for g in range(1, groups):
        send_own(g)

    def piece(owner, h):
        col = pl.multiple_of((owner * heads + h) * HEAD, HEAD)
        return out.at[:, pl.ds(col, HEAD)]

    def x_copy(k, h, owner):
        return pltpu.make_async_remote_copy(
            src_ref=piece(owner, h), dst_ref=piece(owner, h),
            send_sem=x_send.at[k - 1, h], recv_sem=x_recv.at[k - 1, h],
            device_id=x_dev(k), device_id_type=MESH)

    def c_copy(k, h, owner):
        return pltpu.make_async_remote_copy(
            src_ref=piece(owner, h), dst_ref=piece(owner, h),
            send_sem=c_send.at[k, h], recv_sem=c_recv.at[k, h],
            device_id=sibling, device_id_type=MESH)

    factor = math.log2(math.e) / math.sqrt(HEAD)
    window = WINDOW * rows

    for g in range(groups):
        def arrive(which, g=g):
            for i in range(which * CUTS, (which + 1) * CUTS):
                if i % 2:
                    @pl.when(odd == 0)
                    def _():
                        kv_copy(g, i, 1, 0, 1).wait_recv()
                else:
                    kv_copy(g, i, 1, 0, 1).wait_recv()
                three(g, i).wait_recv()

        arrive(0)

        def one_head(r, _, g=g, late=None):
            h = g * GROUP + r
            qcol = pl.multiple_of(h * HEAD, HEAD)
            ocol = pl.multiple_of((t * heads + h) * HEAD, HEAD)
            keys = kv[g, :, 0].reshape(window, HEAD)
            made = []
            for i in range(2):
                part = slice(i * half, (i + 1) * half)
                q = qv[part, pl.ds(qcol, HEAD)]
                sc = lax.dot_general(q, keys, (((1,), (1,)), ((), ())),
                                     preferred_element_type=jnp.float32)
                sc = sc + bias[part, :]
                top = jnp.max(sc, axis=1, keepdims=True)
                w = jnp.exp2((sc - top) * factor)
                total = jnp.sum(w, axis=1, keepdims=True)
                made.append((part, w.astype(jnp.bfloat16), total))
            if late is not None:
                late(1)
            vals = kv[g, :, 1].reshape(window, HEAD)
            for part, w, total in made:
                mixed = jnp.dot(w, vals, preferred_element_type=jnp.float32)
                out[part, pl.ds(ocol, HEAD)] = (mixed / total).astype(out.dtype)
            for k in range(1, hops + 1):
                x_copy(k, h, t).start()
            c_copy(0, h, t).start()
            return 0

        one_head(0, 0, late=arrive)
        lax.fori_loop(1, GROUP // 2, one_head, 0)
        if g + 1 < groups:
            send_on(g + 1)
        lax.fori_loop(GROUP // 2, GROUP, one_head, 0)

    def forward(h, _):
        for k in range(1, hops + 1):
            owner = lax.rem(t - 2 * k + T, T)
            x_copy(k, h, owner).wait_recv()
            c_copy(k, h, owner).start()
        return 0

    lax.fori_loop(0, heads, forward, 0)

    def finish(h, _):
        for k in range(hops + 1):
            c_copy(k, h, t).wait()
            if k > 0:
                x_copy(k, h, t).wait_send()
        return 0

    lax.fori_loop(0, heads, finish, 0)
    for g in range(groups):
        for i in range(2 * CUTS):
            kv_copy(g, i, 1, 0, 1).wait_send()
            two(g, i).wait_send()
            if i % 2:
                @pl.when(odd == 1)
                def _():
                    three(g, i).wait_send()
                    kv_copy(g, i, 3, 1, 2, 3).wait_send()
            else:
                three(g, i).wait_send()


def body(n, T, queries, keys, values, block_pos):
    rows = queries.shape[0]
    groups = keys.shape[1] // HEAD
    heads = groups * GROUP
    hops = T // 2 - 1
    dma = pltpu.SemaphoreType.DMA
    return pl.pallas_call(
        functools.partial(kernel, n, T, rows, groups),
        out_shape=jax.ShapeDtypeStruct((rows, queries.shape[1] * T), jnp.bfloat16),
        in_specs=[pl.BlockSpec(memory_space=pltpu.HBM)] * 4,
        out_specs=pl.BlockSpec(memory_space=pltpu.VMEM),
        scratch_shapes=[
            pltpu.SMEM(block_pos.shape, jnp.int32),
            pltpu.VMEM((rows, heads * HEAD), jnp.bfloat16),
            pltpu.VMEM((groups, WINDOW, 2, rows, HEAD), jnp.bfloat16),
            pltpu.VMEM((rows, WINDOW * rows), jnp.float32),
            dma((groups + 1, 2)),
            dma((groups, 2 * CUTS, 4)),
            dma((groups, 2 * CUTS, 3)),
            dma((hops, heads)),
            dma((hops, heads)),
            dma((hops + 1, heads)),
            dma((hops + 1, heads)),
        ],
        compiler_params=pltpu.CompilerParams(
            collective_id=0, has_side_effects=True, vmem_limit_bytes=32 * 1024 * 1024),
    )(*(pltpu.with_memory_space_constraint(z, pltpu.HBM)
        for z in (queries, keys, values, block_pos)))


def solution(mesh):
    n, T = mesh.shape["seq"], mesh.shape["tensor"]
    placed = (P("seq", "tensor"), P("seq", "tensor"), P("seq", "tensor"), P())
    return jax.shard_map(functools.partial(body, n, T), mesh=mesh, in_specs=placed,
                         out_specs=P("seq", None), check_vma=False)
```
